128 devices in a mesh: src: 8 (over x_lo, y), col: 16 (over x_hi, z, core).
Axes of the slice: x: 4 (x_hi: 2, x_lo: 2; x = x_hi * 2 + x_lo), y: 4, z: 4, core: 2. Of those that a mesh axis runs over, the one named last changes fastest.
Arguments:
- saved_tables: float32 [8, 65536, 256], P('src', 'col'), may hold values from -6 to 6
- saved_state: float32 [8, 65536], P('src', 'col'), may hold values from 0.05 to 4
- slot_table: int32 [8], replicated, may hold values from 0 to 7, each once
- row_ids: int32 [8, 2048], replicated, may hold values from 0 to 65535
- grads: float32 [8, 256, 2048], P('src', 'col'), may hold values from -6 to 6
Outputs:
- tables_out: float32 [8, 256, 65536], P('src', 'col')
- state_out: float32 [8, 65536], P('src')
The draws below stay inside these ranges and needn't reach their ends.
Inputs may be any that keep to these rules, and one draw needn't show every extreme that they name: `slot_table`: each table is in exactly one slot. `row_ids`: row ids may repeat.
All inputs are finite; a program needn't handle non-finite values.
Results may differ from the reference program's by a relative error of at most 0.00002.
Values sent between devices are 32-bit elements; how exact they have to be, the bound alone decides.
No kernel may reach another device: no remote copies, remote signals or barrier semaphores. Data moves between devices by JAX's collectives and lax.ppermute only.
A program may use at most 192 MiB of HBM per device.

```python
import math
import jax
import jax.numpy as jnp
import numpy as np
from jax import lax

D = 256
UPD = 2048
NT = 8
ROWS = 65536


def plant(drawn, rng, smallest, top_value):
    place = [jax.random.randint(jax.random.fold_in(rng, axis), (), 0, length) for axis, length in enumerate(drawn.shape)]
    main_axis = drawn.shape.index(max(drawn.shape))
    beside = place[:main_axis] + [(place[main_axis] + 1) % drawn.shape[main_axis]] + place[main_axis + 1:]
    return drawn.at[tuple(place)].set(smallest).at[tuple(beside)].set(top_value)


def levels(own_key, shape, split, least, top_value):
    gain, own = 1.0, jax.random.fold_in(own_key, 6)
    for dim, parts in split:
        steps = jnp.exp(jax.random.uniform(jax.random.fold_in(own, dim), (parts,), jnp.float32, least / len(split), top_value / len(split)))
        gain = gain * jnp.repeat(steps, shape[dim] // parts).reshape([-1 if axis == dim else 1 for axis in range(len(shape))])
    return gain


def cumulative_ranks(number_of, lean):
    weights = [(1 << 20) // math.isqrt(standing ** lean) + 1 for standing in range(1, number_of + 1)]
    deviation = 1 + sum(weights) // (1 << 30)
    return np.cumsum(np.array([max(1, weight // deviation) for weight in weights]))


def ranked_ids(stream_key, extent, count, slope):
    grid = cumulative_ranks(count, slope)
    ticket = jax.random.randint(jax.random.fold_in(stream_key, 1), extent, 0, int(grid[count - 1]))
    grade = jnp.searchsorted(jnp.asarray(grid, jnp.int32), ticket, side="right")
    return jax.random.permutation(jax.random.fold_in(stream_key, 2), count)[grade].astype(jnp.int32)


def gaussian(stream_key, dims, scale, reach, shards=(), held_as=jnp.bfloat16):
    factor_of = levels(stream_key, dims, shards, -0.22, 0.18) if shards else 1.0
    values = jax.random.normal(stream_key, dims, jnp.float32) * scale * factor_of
    return jnp.minimum(jnp.maximum(values, -reach), reach).astype(held_as)


def setup_inputs(seed: int = 0) -> dict:
    streams_of = jax.random.split(jax.random.key(seed), 6)
    saved_tables = gaussian(streams_of[0], (NT, ROWS, D), 1.0, 6.0, ((0, 8), (1, 16)), jnp.float32)
    saved_state = jnp.clip(jnp.exp(math.log(4.0) - 4.3820266 * jax.random.uniform(streams_of[1], (NT, ROWS), jnp.float32) ** levels(streams_of[1], (NT, ROWS), ((0, 8), (1, 16)), -0.2, 0.2)), 0.05, 4.0)
    slot_table = jax.random.permutation(streams_of[2], NT).astype(jnp.int32)
    row_ids = plant(ranked_ids(streams_of[3], (NT, UPD), ROWS, 2), jax.random.fold_in(streams_of[3], 3), 0, ROWS - 1).astype(jnp.int32)
    grads = gaussian(streams_of[4], (NT, D, UPD), 1.0, 6.0, ((0, 8), (1, 16)), jnp.float32)
    return {"saved_tables": saved_tables, "saved_state": saved_state, "slot_table": slot_table, "row_ids": row_ids, "grads": grads}


learn_rate = 0.5
epsilon = 1e-08

def reference(saved_tables, saved_state, slot_table, row_ids, grads):

    def one_slot(slot):
        table = slot_table[slot]
        weights = saved_tables[slot]
        state = saved_state[slot]
        summed = jnp.zeros((ROWS, D), jnp.float32).at[row_ids[table]].add(grads[table].T)
        new_state = state + lax.optimization_barrier(jnp.sum(summed * summed, axis=1)) / D
        new_weights = weights - learn_rate * summed / (jnp.sqrt(new_state)[:, None] + epsilon)
        return (new_weights.T, new_state)
    result = lax.map(one_slot, jnp.arange(NT, dtype=jnp.int32))
    return (result[0], result[1])
```

```python
import jax
import jax.numpy as jnp
from jax import lax
from jax.experimental import pallas as pl
from jax.experimental.pallas import tpu as pltpu
from jax.sharding import Mesh
from jax.sharding import PartitionSpec as P

D = 256
UPD = 2048
ROWS = 65536
LEARN_RATE = 0.5
EPSILON = 1e-08
F32 = jnp.float32
AXES = ("xl", "y", "xh", "z", "core")
SHAPE = (2, 4, 2, 4, 2)
SRC = ("xl", "y")
COL = ("xh", "z", "core")
VMEM = pltpu.VMEM
CHUNK, BLOCK, CARRY = 136, 544, 16


def params():
    return pltpu.CompilerParams(vmem_limit_bytes=40 * 1024 * 1024)


def cost(us):
    return pl.CostEstimate(flops=int(us * 2e6), bytes_accessed=1000000, transcendentals=0)


def shift(array, dxl=0, dy=0, dxh=0, dz=0, dcore=0):
    step = (dxl, dy, dxh, dz, dcore)
    pairs = []
    for source in range(128):
        at, rest = [], source
        for size in reversed(SHAPE):
            at.append(rest % size)
            rest //= size
        target = 0
        for place, size, by in zip(reversed(at), SHAPE, step):
            target = target * size + (place + by) % size
        pairs.append((source, target))
    return lax.ppermute(array, AXES, pairs)


def pack_kernel(pick_ref, table_ref, state_ref, *rest):
    outs, turned = rest[:-1], rest[-1]
    for b in range(8):
        turned[:, b * 128 : (b + 1) * 128] = table_ref[0, b * 128 : (b + 1) * 128, :].T
    for o, out in enumerate(outs):
        first = pl.multiple_of(pick_ref[1 + o] * 16, 16)
        for a in range(2):
            rows = turned[pl.ds(first + 8 * a, 8), :]
            for b in range(8):
                out[(b * 2 + a) * 8 : (b * 2 + a) * 8 + 8, :] = rows[:, b * 128 : (b + 1) * 128]
        out[128:136, :] = state_ref[...]


def pack(table, state, pick, sizes):
    spec = pltpu.PrefetchScalarGridSpec(
        num_scalar_prefetch=1,
        grid=(4,),
        in_specs=[
            pl.BlockSpec((1, 1024, 128), lambda i, p: (0, i, p[0])),
            pl.BlockSpec((8, 128), lambda i, p: (i, 0)),
        ],
        out_specs=[pl.BlockSpec((CHUNK, 128), lambda i, p: (i, 0)) for _ in sizes],
        scratch_shapes=[VMEM((128, 1024), F32)],
    )
    return pl.pallas_call(
        pack_kernel,
        grid_spec=spec,
        out_shape=[jax.ShapeDtypeStruct((size, 128), F32) for size in sizes],
        compiler_params=params(),
        cost_estimate=cost(3),
        name="pack",
    )(pick, table, state)


def merge_kernel(pick_ref, ids_ref, g0, g1, g2, g3, rows_ref, square_ref, idc, equal, total):
    which = pick_ref[0]
    g = jnp.where(which == 0, g0[...], g1[...])
    g = jnp.where(which == 2, g2[...], g)
    g = jnp.where(which == 3, g3[...], g)
    high = g.astype(jnp.bfloat16)
    left = g - high.astype(F32)
    middle = left.astype(jnp.bfloat16)
    low = (left - middle.astype(F32)).astype(jnp.bfloat16)
    terms = jnp.concatenate([high, middle, low], axis=0)
    for i in range(16):
        idc[i * 128 : (i + 1) * 128, :] = jnp.broadcast_to(ids_ref[i : i + 1, :], (128, 128)).T
    for n in range(8):
        for m in range(2):
            row = ids_ref[2 * n + m : 2 * n + m + 1, :]
            same = jnp.where(idc[...] == row, 1.0, 0.0)
            equal[:, m * 128 : (m + 1) * 128] = same.astype(jnp.bfloat16)
        sums = jnp.dot(terms, equal[...], preferred_element_type=F32)
        total[:, n * 256 : (n + 1) * 256] = sums[0:16] + sums[16:32] + sums[32:48]
    for i in range(16):
        s = total[:, i * 128 : (i + 1) * 128]
        square_ref[i : i + 1, :] = jnp.sum(s * s, axis=0, keepdims=True)
        rows_ref[i * 128 : (i + 1) * 128, :] = jnp.concatenate([s] * 8, axis=0).T


def merge(pick, ids, grads):
    return pl.pallas_call(
        merge_kernel,
        in_specs=[pl.BlockSpec(memory_space=pltpu.SMEM)] + [pl.BlockSpec(memory_space=VMEM)] * 5,
        out_specs=[pl.BlockSpec(memory_space=VMEM)] * 2,
        out_shape=[jax.ShapeDtypeStruct((UPD, 128), F32), jax.ShapeDtypeStruct((16, 128), F32)],
        scratch_shapes=[VMEM((UPD, 128), F32), VMEM((UPD, 256), jnp.bfloat16), VMEM((16, UPD), F32)],
        compiler_params=params(),
        cost_estimate=cost(4),
        name="merge",
    )(pick, ids, *grads)


def place_kernel(ids_ref, rows_ref, sums_ref, at_ref):
    sums_ref[...] = jnp.zeros_like(sums_ref)
    at_ref[...] = jnp.full_like(at_ref, -1)
    lane = lax.broadcasted_iota(jnp.int32, (1, 128), 1)
    group = lane >> 4

    def step(t, carry):
        for u in range(8):
            j = t * 8 + u
            r = ids_ref[j]
            row = ((r >> 10) << 7) | (r & 127)
            value = rows_ref[pl.ds(j, 1), :]
            pltpu.store(sums_ref.at[pl.ds(row, 1), :], value, mask=group == ((r >> 7) & 7))
            here = jnp.full((1, 128), j, jnp.int32)
            pltpu.store(at_ref.at[pl.ds(r >> 7, 1), :], here, mask=lane == (r & 127))
        return carry

    lax.fori_loop(0, UPD // 8, step, 0)


def place(ids, rows):
    return pl.pallas_call(
        place_kernel,
        in_specs=[pl.BlockSpec(memory_space=pltpu.SMEM), pl.BlockSpec(memory_space=VMEM)],
        out_specs=[pl.BlockSpec(memory_space=VMEM)] * 2,
        out_shape=[
            jax.ShapeDtypeStruct((ROWS // 8, 128), F32),
            jax.ShapeDtypeStruct((ROWS // 128, 128), jnp.int32),
        ],
        compiler_params=params(),
        cost_estimate=cost(9),
        name="place",
    )(ids, rows)


def attach_kernel(mine, other, *rest):
    n = (len(rest) - 3) // 2
    outs, chip_ref, held, sem = rest[n : 2 * n], rest[-3], rest[-2], rest[-1]
    held[...] = mine[...] + other[...]
    chip_ref[...] = held[...]
    copies = [
        pltpu.make_async_copy(held, out.at[pl.ds(BLOCK, CARRY), :], sem.at[i])
        for i, out in enumerate(outs)
    ]
    for copy in copies:
        copy.start()
    for copy in copies:
        copy.wait()


def attach(mine, other, blocks):
    n = len(blocks)
    outs = pl.pallas_call(
        attach_kernel,
        in_specs=[pl.BlockSpec(memory_space=VMEM)] * 2 + [pl.BlockSpec(memory_space=pl.ANY)] * n,
        out_specs=[pl.BlockSpec(memory_space=pl.ANY)] * n + [pl.BlockSpec(memory_space=VMEM)],
        out_shape=[jax.ShapeDtypeStruct(b.shape, F32) for b in blocks]
        + [jax.ShapeDtypeStruct((16, 128), F32)],
        scratch_shapes=[VMEM((CARRY, 128), F32), pltpu.SemaphoreType.DMA((n,))],
        input_output_aliases={2 + i: i for i in range(n)},
        compiler_params=params(),
        cost_estimate=cost(1),
        name="attach",
    )(mine, other, *blocks)
    return outs[:-1], outs[-1]


def total_kernel(chip_ref, own, *rest):
    blocks, out, held, sem = rest[:-3], rest[-3], rest[-2], rest[-1]
    copies = [
        pltpu.make_async_copy(b.at[pl.ds(BLOCK, CARRY), :], held.at[chip_ref[1 + i]], sem.at[i])
        for i, b in enumerate(blocks)
    ]
    for copy in copies:
        copy.start()
    held[chip_ref[0]] = own[...]
    for copy in copies:
        copy.wait()
    total = held[0]
    for i in range(1, 8):
        total = total + held[i]
    out[...] = total


def total_of(chips, own, blocks):
    return pl.pallas_call(
        total_kernel,
        in_specs=[pl.BlockSpec(memory_space=pltpu.SMEM), pl.BlockSpec(memory_space=VMEM)]
        + [pl.BlockSpec(memory_space=pl.ANY)] * len(blocks),
        out_specs=pl.BlockSpec(memory_space=VMEM),
        out_shape=jax.ShapeDtypeStruct((16, 128), F32),
        scratch_shapes=[VMEM((8, CARRY, 128), F32), pltpu.SemaphoreType.DMA((len(blocks),))],
        compiler_params=params(),
        cost_estimate=cost(1),
        name="total",
    )(chips, own, *blocks)


def finish_kernel(n, alias, from_ref, sums_ref, at_ref, total_ref, *rest):
    blocks = rest[:n]
    rest = rest[n + (2 if alias else 0) :]
    out_ref, state_out, table, state, sems = rest
    waits = [None, None]
    for k, block in enumerate(blocks):
        slot = k % 2
        if waits[slot] is not None:
            for copy in waits[slot]:
                copy.wait()
        source = from_ref[k]

        def chunk(i, carry):
            part = source * 4 + i
            at = at_ref[pl.ds(pl.multiple_of(part * 8, 8), 8), :]
            high, low = at >> 7, at & 127
            total = jnp.zeros((8, 128), F32)
            for h in range(16):
                row = jnp.broadcast_to(total_ref[h : h + 1, :], (8, 128))
                total = jnp.where(high == h, jnp.take_along_axis(row, low, axis=1), total)
            base = pl.multiple_of(i * CHUNK, 8)
            new = block[pl.ds(base + 128, 8), :] + total / D
            state[slot, pl.ds(pl.multiple_of(i * 8, 8), 8), :] = new
            scale = LEARN_RATE / (jnp.sqrt(new) + EPSILON)
            sums = sums_ref[pl.ds(pl.multiple_of(part * 128, 128), 128), :].T
            for q in range(8):
                rate = scale[q : q + 1, :]
                for a in range(2):
                    old = block[pl.ds(base + (q * 2 + a) * 8, 8), :]
                    value = old - sums[q * 16 + a * 8 : q * 16 + a * 8 + 8, :] * rate
                    lanes = pl.ds(pl.multiple_of(i * 1024 + q * 128, 128), 128)
                    table[slot, a * 8 : a * 8 + 8, lanes] = value
            return carry

        lax.fori_loop(0, 4, chunk, 0)
        columns = pl.ds(pl.multiple_of(source * 4096, 4096), 4096)
        rows = pl.ds(pl.multiple_of(source * 32, 32), 32)
        waits[slot] = [
            pltpu.make_async_copy(table.at[slot], out_ref.at[0, :, columns], sems.at[slot, 0]),
            pltpu.make_async_copy(state.at[slot], state_out.at[rows, :], sems.at[slot, 1]),
        ]
        for copy in waits[slot]:
            copy.start()
    for copies in waits:
        for copy in copies or ():
            copy.wait()


def finish(sources, sums, at, total, blocks, outs):
    n, alias = len(blocks), outs is not None
    first = 4 + n
    anywhere = pl.BlockSpec(memory_space=pl.ANY)
    return pl.pallas_call(
        lambda *refs: finish_kernel(n, alias, *refs),
        in_specs=[pl.BlockSpec(memory_space=pltpu.SMEM)]
        + [pl.BlockSpec(memory_space=VMEM)] * (3 + n)
        + [anywhere] * (2 if alias else 0),
        out_specs=[anywhere] * 2,
        out_shape=[
            jax.ShapeDtypeStruct((1, 16, ROWS), F32),
            jax.ShapeDtypeStruct((ROWS // 128, 128), F32),
        ],
        scratch_shapes=[
            VMEM((2, 16, 4096), F32),
            VMEM((2, 32, 128), F32),
            pltpu.SemaphoreType.DMA((2, 2)),
        ],
        input_output_aliases={first: 0, first + 1: 1} if alias else {},
        compiler_params=params(),
        cost_estimate=cost(0.4 * n),
        name="finish",
    )(sources, sums, at, total, *blocks, *(outs or ()))


def after(array, *others):
    return lax.optimization_barrier((array, *others))[0]


def ints(*values):
    return jnp.stack([jnp.asarray(v, jnp.int32) for v in values])


def body(saved_tables, saved_state, slot_table, row_ids, grads):
    xl, y, xh, z, core = (lax.axis_index(a) for a in AXES)
    table = slot_table[xl * 4 + y]
    ids = lax.dynamic_index_in_dim(row_ids, table, 0, keepdims=False)
    state = saved_state.reshape(32, 128)

    own = grads[0]
    near = shift(own, dxl=1)
    far_pick = ints(1 - xh, *(((z + o // 2) % 4) * 2 + (core + o) % 2 for o in range(8)))
    far = pack(saved_tables, state, far_pick, [BLOCK + CARRY * (1 - o % 2) for o in range(8)])
    near_pick = far_pick.at[0].set(xh)
    home = pack(saved_tables, state, near_pick, [BLOCK + CARRY * (o in (2, 4, 6)) for o in range(8)])

    def wanted(dy):
        return jnp.where(slot_table[xl * 4 + (y + dy) % 4] // 4 == xl, own, near)

    pieces = [wanted(0)] + [shift(wanted(dy), dy=dy) for dy in (1, 2, 3)]

    first = [(1, 2), (0, 2), (1, 1), (0, 1), (1, 3), (0, 3), (1, 0), (0, 0)]
    came = {}
    for dx, dz in first:
        block = (far if dx else home)[dz * 2 + 1]
        came[dx, dz, 1] = shift(block, dxh=dx, dz=dz, dcore=1)
    came[0, 0, 0] = home[0]

    from_y = (y - table % 4) % 4
    ids_f = ids.astype(F32).reshape(16, 128)
    rows, squares = merge(ints(from_y), ids_f, pieces)
    other = shift(squares, dcore=1)
    second = [(1, 2), (0, 2), (1, 1), (0, 1), (1, 3), (0, 3), (1, 0)]
    blocks, chip = attach(squares, other, [(far if dx else home)[dz * 2] for dx, dz in second])
    for (dx, dz), block in zip(second, blocks):
        came[dx, dz, 0] = shift(block, dxh=dx, dz=dz)
    sums, at = place(ids, rows)

    chips = ints(xh * 4 + z, *(((xh + dx) % 2) * 4 + (z - dz) % 4 for dx, dz in second))
    total = total_of(chips, chip, [came[dx, dz, 0] for dx, dz in second])

    def finished(flows, outs):
        sources = ints(
            *((((xh + dx) % 2) * 4 + (z - dz) % 4) * 2 + (core + dc) % 2 for dx, dz, dc in flows)
        )
        return finish(sources, sums, at, total, [came[f] for f in flows], outs)

    early = [(0, 0, 0)] + [(dx, dz, 1) for dx, dz in first]
    late = [(dx, dz, 0) for dx, dz in second]
    outs = finished(early, None)
    outs = finished(late, outs)
    return outs[0], outs[1].reshape(1, ROWS)


def solution(mesh):
    torus = Mesh(mesh.devices.reshape(SHAPE), AXES)
    in_specs = (P(SRC, COL, None), P(SRC, COL), P(), P(), P(SRC, COL, None))
    out_specs = (P(SRC, COL, None), P(SRC, None))
    return jax.shard_map(body, mesh=torus, in_specs=in_specs, out_specs=out_specs, check_vma=False)
```

```python
import functools

import jax
import jax.numpy as jnp
from jax import lax
from jax.experimental import pallas as pl
from jax.experimental.pallas import tpu as pltpu
from jax.sharding import Mesh
from jax.sharding import PartitionSpec as P


D = 256
UPD = 2048
ROWS = 65536
LEARN_RATE = 0.5
EPSILON = 1e-08
F32 = jnp.float32
AXES = ("xl", "y", "xh", "z", "core")
SHAPE = (2, 4, 2, 4, 2)
SRC = ("xl", "y")
COL = ("xh", "z", "core")
VMEM = pltpu.VMEM
CHUNK, BLOCK, CARRY = 136, 544, 16


def params():
    return pltpu.CompilerParams(vmem_limit_bytes=40 * 1024 * 1024)


def cost(us):
    return pl.CostEstimate(flops=int(us * 2e6), bytes_accessed=1000000, transcendentals=0)


def shift(array, dxl=0, dy=0, dxh=0, dz=0, dcore=0):
    step = (dxl, dy, dxh, dz, dcore)
    pairs = []
    for source in range(128):
        at, rest = [], source
        for size in reversed(SHAPE):
            at.append(rest % size)
            rest //= size
        target = 0
        for place, size, by in zip(reversed(at), SHAPE, step):
            target = target * size + (place + by) % size
        pairs.append((source, target))
    return lax.ppermute(array, AXES, pairs)


def coordinates(ref):
    at = ref[0]
    return at >> 6, (at >> 4) & 3, (at >> 3) & 1, (at >> 1) & 3, at & 1


def source_of(ref, dx, dz, dc):
    _, _, xh, z, core = coordinates(ref)
    return (((xh + dx) & 1) * 4 + ((z - dz) & 3)) * 2 + ((core + dc) & 1)


def pack_kernel(here_ref, table_hbm, state_hbm, *rest):
    outs, held, state, turned, sem = rest[:16], *rest[16:]
    _, _, xh, z, core = coordinates(here_ref)
    copies = [pltpu.make_async_copy(state_hbm, state, sem.at[8])]
    for k in range(8):
        half = 1 - xh if k < 4 else xh
        columns = pl.ds(pl.multiple_of(half * 128, 128), 128)
        rows = pl.ds(k % 4 * 1024, 1024)
        copies.append(pltpu.make_async_copy(table_hbm.at[0, rows, columns], held.at[k], sem.at[k]))
    for copy in copies:
        copy.start()
    copies[0].wait()
    for k in range(8):
        copies[1 + k].wait()
        for b in range(8):
            turned[k, :, b * 128 : (b + 1) * 128] = held[k, b * 128 : (b + 1) * 128, :].T
        i = k % 4
        for o, out in enumerate(outs[:8] if k < 4 else outs[8:]):
            first = pl.multiple_of((((z + o // 2) & 3) * 2 + ((core + o) & 1)) * 16, 16)
            for a in range(2):
                rows = turned[k, pl.ds(first + 8 * a, 8), :]
                for b in range(8):
                    at = i * CHUNK + (b * 2 + a) * 8
                    out[at : at + 8, :] = rows[:, b * 128 : (b + 1) * 128]
            out[i * CHUNK + 128 : (i + 1) * CHUNK, :] = state[i * 8 : i * 8 + 8, :]


def pack(here, table, state, sizes):
    hbm = pl.BlockSpec(memory_space=pltpu.HBM)
    return pl.pallas_call(
        pack_kernel,
        in_specs=[pl.BlockSpec(memory_space=pltpu.SMEM), hbm, hbm],
        out_specs=[pl.BlockSpec(memory_space=VMEM)] * len(sizes),
        out_shape=[jax.ShapeDtypeStruct((size, 128), F32) for size in sizes],
        scratch_shapes=[
            VMEM((8, 1024, 128), F32),
            VMEM((32, 128), F32),
            VMEM((8, 128, 1024), F32),
            pltpu.SemaphoreType.DMA((9,)),
        ],
        compiler_params=pltpu.CompilerParams(vmem_limit_bytes=LIMIT),
        cost_estimate=cost(4),
        name="pack",
    )(here, table, state)


LIMIT = 50000000


def choose_kernel(here_ref, slots_ref, ids_hbm, own_hbm, near, w0, w1, w2, w3, out_ref, row_ref, *rest):
    ids, own, sem = rest
    copies = [
        pltpu.make_async_copy(own_hbm.at[0], own, sem.at[0]),
        pltpu.make_async_copy(ids_hbm, ids, sem.at[1]),
    ]
    for copy in copies:
        copy.start()
    for copy in copies:
        copy.wait()
    xl, y, _, _, _ = coordinates(here_ref)
    for dy, out in enumerate((w0, w1, w2, w3)):
        table = slots_ref[xl * 4 + ((y + dy) & 3)]
        out[...] = jnp.where(table >> 2 == xl, own[...], near[0])
    row = ids[pl.ds(slots_ref[xl * 4 + y], 1), :]
    for i in range(16):
        part = row[:, i * 128 : (i + 1) * 128]
        out_ref[i : i + 1, :] = part
        row_ref[i : i + 1, :] = ((part >> 10) << 7) | (part & 127)


def choose(here, slots, ids, own, near):
    smem = pl.BlockSpec(memory_space=pltpu.SMEM)
    vmem = pl.BlockSpec(memory_space=VMEM)
    hbm = pl.BlockSpec(memory_space=pltpu.HBM)
    return pl.pallas_call(
        choose_kernel,
        in_specs=[smem] * 2 + [hbm] * 2 + [vmem],
        out_specs=[vmem] * 6,
        out_shape=[jax.ShapeDtypeStruct((16, UPD), F32)] * 4
        + [jax.ShapeDtypeStruct((16, 128), jnp.int32)] * 2,
        scratch_shapes=[
            VMEM((8, UPD), jnp.int32),
            VMEM((16, UPD), F32),
            pltpu.SemaphoreType.DMA((2,)),
        ],
        compiler_params=params(),
        cost_estimate=cost(1),
        name="choose",
    )(here, slots, ids, own, near)


def merge_kernel(here_ref, slots_ref, int_ids_ref, g0, g1, g2, g3, rows_ref, square_ref, ids_ref, idc, equal, total):
    xl, y, _, _, _ = coordinates(here_ref)
    which = (y - slots_ref[xl * 4 + y]) & 3
    ids_ref[...] = int_ids_ref[...].astype(F32)
    g = jnp.where(which == 0, g0[...], g1[...])
    g = jnp.where(which == 2, g2[...], g)
    g = jnp.where(which == 3, g3[...], g)
    high = g.astype(jnp.bfloat16)
    left = g - high.astype(F32)
    middle = left.astype(jnp.bfloat16)
    low = (left - middle.astype(F32)).astype(jnp.bfloat16)
    terms = jnp.concatenate([high, middle, low], axis=0)
    for i in range(16):
        idc[i * 128 : (i + 1) * 128, :] = jnp.broadcast_to(ids_ref[i : i + 1, :], (128, 128)).T
    for n in range(8):
        for m in range(2):
            row = ids_ref[2 * n + m : 2 * n + m + 1, :]
            same = jnp.where(idc[...] == row, 1.0, 0.0)
            equal[:, m * 128 : (m + 1) * 128] = same.astype(jnp.bfloat16)
        sums = jnp.dot(terms, equal[...], preferred_element_type=F32)
        total[:, n * 256 : (n + 1) * 256] = sums[0:16] + sums[16:32] + sums[32:48]
    for i in range(16):
        s = total[:, i * 128 : (i + 1) * 128]
        square_ref[i : i + 1, :] = jnp.sum(s * s, axis=0, keepdims=True)
        rows_ref[i * 128 : (i + 1) * 128, :] = jnp.concatenate([s] * 8, axis=0).T


def merge(here, slots, ids, grads):
    return pl.pallas_call(
        merge_kernel,
        in_specs=[pl.BlockSpec(memory_space=pltpu.SMEM)] * 2 + [pl.BlockSpec(memory_space=VMEM)] * 5,
        out_specs=[pl.BlockSpec(memory_space=VMEM)] * 2,
        out_shape=[jax.ShapeDtypeStruct((UPD, 128), F32), jax.ShapeDtypeStruct((16, 128), F32)],
        scratch_shapes=[
            VMEM((16, 128), F32),
            VMEM((UPD, 128), F32),
            VMEM((UPD, 256), jnp.bfloat16),
            VMEM((16, UPD), F32),
        ],
        compiler_params=params(),
        cost_estimate=cost(4),
        name="merge",
    )(here, slots, ids, *grads)


def place_kernel(ids_ref, at_row_ref, rows_ref, turned_ref, at_ref, sums_ref):
    sums_ref[...] = jnp.zeros_like(sums_ref)
    at_ref[...] = jnp.full_like(at_ref, -1)
    lane = lax.broadcasted_iota(jnp.int32, (1, 128), 1)
    group = (lane >> 4) << 7

    def step(i, carry):
        first = jnp.full((1, 128), i * 128, jnp.int32)
        for u in range(128):
            r = ids_ref[i, u]
            all_r = jnp.full((1, 128), r, jnp.int32)
            value = rows_ref[pl.ds(i * 128 + u, 1), :]
            here = sums_ref.at[pl.ds(at_row_ref[i, u], 1), :]
            pltpu.store(here, value, mask=group == (all_r & 0x380))
            pltpu.store(at_ref.at[pl.ds(r >> 7, 1), :], first + u, mask=lane == (all_r & 127))
        return carry

    lax.fori_loop(0, 16, step, 0)

    def turn(i, carry):
        for u in range(8):
            part = pl.ds(pl.multiple_of((i * 8 + u) * 128, 128), 128)
            turned_ref[part, :] = sums_ref[part, :].T
        return carry

    lax.fori_loop(0, 8, turn, 0)


def place(ids, at_rows, rows):
    return pl.pallas_call(
        place_kernel,
        in_specs=[pl.BlockSpec(memory_space=pltpu.SMEM)] * 2 + [pl.BlockSpec(memory_space=VMEM)],
        out_specs=[pl.BlockSpec(memory_space=VMEM)] * 2,
        out_shape=[
            jax.ShapeDtypeStruct((ROWS // 8, 128), F32),
            jax.ShapeDtypeStruct((ROWS // 128, 128), jnp.int32),
        ],
        scratch_shapes=[VMEM((ROWS // 8, 128), F32)],
        compiler_params=params(),
        cost_estimate=cost(6),
        name="place",
    )(ids, at_rows, rows)


def attach_kernel(mine, other, *rest):
    n = (len(rest) - 3) // 2
    outs, chip_ref, held, sem = rest[n : 2 * n], rest[-3], rest[-2], rest[-1]
    held[...] = mine[...] + other[...]
    chip_ref[...] = held[...]
    copies = [
        pltpu.make_async_copy(held, out.at[pl.ds(BLOCK, CARRY), :], sem.at[i])
        for i, out in enumerate(outs)
    ]
    for copy in copies:
        copy.start()
    for copy in copies:
        copy.wait()


def attach(mine, other, blocks):
    n = len(blocks)
    outs = pl.pallas_call(
        attach_kernel,
        in_specs=[pl.BlockSpec(memory_space=VMEM)] * 2 + [pl.BlockSpec(memory_space=pl.ANY)] * n,
        out_specs=[pl.BlockSpec(memory_space=pl.ANY)] * n + [pl.BlockSpec(memory_space=VMEM)],
        out_shape=[jax.ShapeDtypeStruct(b.shape, F32) for b in blocks]
        + [jax.ShapeDtypeStruct((16, 128), F32)],
        scratch_shapes=[VMEM((CARRY, 128), F32), pltpu.SemaphoreType.DMA((n,))],
        input_output_aliases={2 + i: i for i in range(n)},
        compiler_params=params(),
        cost_estimate=cost(1),
        name="attach",
    )(mine, other, *blocks)
    return outs[:-1], outs[-1]


def total_kernel(flows, here_ref, own, *rest):
    blocks, out, held, sem = rest[:-3], rest[-3], rest[-2], rest[-1]
    copies = [
        pltpu.make_async_copy(b.at[pl.ds(BLOCK, CARRY), :], held.at[source_of(here_ref, *flows[i]) >> 1], sem.at[i])
        for i, b in enumerate(blocks)
    ]
    for copy in copies:
        copy.start()
    held[source_of(here_ref, 0, 0, 0) >> 1] = own[...]
    for copy in copies:
        copy.wait()
    total = held[0]
    for i in range(1, 8):
        total = total + held[i]
    out[...] = total


def total_of(here, own, flows, blocks):
    return pl.pallas_call(
        functools.partial(total_kernel, flows),
        in_specs=[pl.BlockSpec(memory_space=pltpu.SMEM), pl.BlockSpec(memory_space=VMEM)]
        + [pl.BlockSpec(memory_space=pl.ANY)] * len(blocks),
        out_specs=pl.BlockSpec(memory_space=VMEM),
        out_shape=jax.ShapeDtypeStruct((16, 128), F32),
        scratch_shapes=[VMEM((8, CARRY, 128), F32), pltpu.SemaphoreType.DMA((len(blocks),))],
        compiler_params=params(),
        cost_estimate=cost(1),
        name="total",
    )(here, own, *blocks)


def finish_kernel(flows, alias, here_ref, sums_ref, at_ref, total_ref, *rest):
    n = len(flows)
    blocks = rest[:n]
    rest = rest[n + (2 if alias else 0) :]
    out_ref, state_out, table, state, sems = rest
    copies = []
    for k, block in enumerate(blocks):
        source = source_of(here_ref, *flows[k])

        def chunk(i, carry):
            part = source * 4 + i
            at = at_ref[pl.ds(pl.multiple_of(part * 8, 8), 8), :]
            high, low = at >> 7, at & 127
            total = jnp.zeros((8, 128), F32)
            for h in range(16):
                row = jnp.broadcast_to(total_ref[h : h + 1, :], (8, 128))
                total = jnp.where(high == h, jnp.take_along_axis(row, low, axis=1), total)
            base = pl.multiple_of(i * CHUNK, 8)
            new = block[pl.ds(base + 128, 8), :] + total / D
            state[k, pl.ds(pl.multiple_of(i * 8, 8), 8), :] = new
            scale = LEARN_RATE / (jnp.sqrt(new) + EPSILON)
            first = pl.multiple_of(part * 128, 128)
            for q in range(8):
                rate = scale[q : q + 1, :]
                for a in range(2):
                    old = block[pl.ds(base + (q * 2 + a) * 8, 8), :]
                    value = old - sums_ref[pl.ds(first + q * 16 + a * 8, 8), :] * rate
                    lanes = pl.ds(pl.multiple_of(i * 1024 + q * 128, 128), 128)
                    table[k, a * 8 : a * 8 + 8, lanes] = value
            return carry

        lax.fori_loop(0, 4, chunk, 0, unroll=True)
        columns = pl.ds(pl.multiple_of(source * 4096, 4096), 4096)
        rows = pl.ds(pl.multiple_of(source * 32, 32), 32)
        for a in range(2):
            half = pl.ds(a * 8, 8)
            copies.append(
                pltpu.make_async_copy(
                    table.at[k, half, :], out_ref.at[0, half, columns], sems.at[k, a]
                )
            )
        copies.append(pltpu.make_async_copy(state.at[k], state_out.at[rows, :], sems.at[k, 2]))
        for copy in copies[-3:]:
            copy.start()
    for copy in copies:
        copy.wait()


def finish(here, sums, at, total, flows, blocks, outs):
    n, alias = len(blocks), outs is not None
    first = 4 + n
    anywhere = pl.BlockSpec(memory_space=pl.ANY)
    return pl.pallas_call(
        functools.partial(finish_kernel, flows, alias),
        in_specs=[pl.BlockSpec(memory_space=pltpu.SMEM)]
        + [pl.BlockSpec(memory_space=VMEM)] * (3 + n)
        + [anywhere] * (2 if alias else 0),
        out_specs=[anywhere] * 2,
        out_shape=[
            jax.ShapeDtypeStruct((1, 16, ROWS), F32),
            jax.ShapeDtypeStruct((ROWS // 128, 128), F32),
        ],
        scratch_shapes=[
            VMEM((n, 16, 4096), F32),
            VMEM((n, 32, 128), F32),
            pltpu.SemaphoreType.DMA((n, 3)),
        ],
        input_output_aliases={first: 0, first + 1: 1} if alias else {},
        compiler_params=params(),
        cost_estimate=cost(0.3 * n),
        name="finish",
    )(here, sums, at, total, *blocks, *(outs or ()))


SECOND = ((1, 2), (0, 2), (1, 1), (0, 1), (1, 3), (0, 3), (1, 0))


def update(saved_tables, saved_state, slot_table, row_ids, grads):
    here = lax.axis_index(AXES).astype(jnp.int32)[None]
    state = saved_state.reshape(32, 128)

    def sent(block, dx, dz, dc):
        return shift(block, dxh=dx, dz=dz, dcore=dc)

    near = shift(grads, dxl=1)
    sizes = [BLOCK + CARRY * (o % 2 == 0 and o != 8) for o in range(16)]
    packed = pack(here, saved_tables, state, sizes)
    far, home = packed[:8], packed[8:]
    *pieces, ids, at_rows = choose(here, slot_table, row_ids, grads, near)
    for dy in (1, 2, 3):
        pieces[dy] = shift(pieces[dy], dy=dy)

    came = {(0, 0, 0): home[0]}
    for dx, dz in (*SECOND, (0, 0)):
        came[dx, dz, 1] = sent((far if dx else home)[dz * 2 + 1], dx, dz, 1)
    rows, squares = merge(here, slot_table, ids, pieces)
    other = shift(squares, dcore=1)
    blocks, chip = attach(squares, other, [(far if dx else home)[dz * 2] for dx, dz in SECOND])
    for (dx, dz), block in zip(SECOND, blocks):
        came[dx, dz, 0] = sent(block, dx, dz, 0)
    sums, at = place(ids, at_rows, rows)
    carried = tuple((dx, dz, 0) for dx, dz in SECOND)
    total = total_of(here, chip, carried, [came[f] for f in carried])

    def finished(flows, outs):
        return finish(here, sums, at, total, flows, [came[f] for f in flows], outs)

    outs = finished(tuple(came), None)
    return outs[0], outs[1].reshape(1, ROWS)


def solution(mesh):
    torus = Mesh(mesh.devices.reshape(SHAPE), AXES)
    in_specs = (P(SRC, COL, None), P(SRC, COL), P(), P(), P(SRC, COL, None))
    out_specs = (P(SRC, COL, None), P(SRC, None))
    return jax.shard_map(update, mesh=torus, in_specs=in_specs, out_specs=out_specs, check_vma=False)
```
